32 devices in a mesh: rep: 8 (over z, y), shard: 4 (over x, core).
Axes of the slice: x: 2, y: 2, z: 4, core: 2. Of those that a mesh axis runs over, the one named last changes fastest.
Arguments:
- activ: bfloat16 [4096, 8192], P(('rep', 'shard')), may hold values from -6 to 6
- key_grad: bfloat16 [4096, 640], P(('rep', 'shard')), may hold values from -1.1953125 to 1.1953125
- key_weight: bfloat16 [8192, 640], P('shard'), may hold values from -0.25 to 0.25
- feedback: bfloat16 [8, 40960, 128], P('rep', 'shard'), may hold values from -24 to 24
- kept: int32 [8, 4, 512], P('rep', 'shard'), may hold values from 0 to 10239, as said below
- region_len: int32 [4, 8], P('shard'), may hold values from 640 to 1920, as said below
Outputs:
- input_grad: bfloat16 [4096, 8192], P(('rep', 'shard'))
- next_feedback: bfloat16 [8, 40960, 128], P('rep', 'shard')
- owned_sum: float32 [4, 15360, 128], P('shard', 'rep')
The draws below stay inside these ranges and needn't reach their ends.
Inputs may be any that keep to these rules, and one draw needn't show every extreme that they name: `region_len`: each row splits its shard's 10240 blocks into 8 regions in order of owner and sums to 10240; every row has a region of exactly 1920 blocks. `kept`: the 512 numbers of a row are different blocks of that shard. At most 128 of them lie in one region of the shard; every row has exactly 128 in some region, and in every shard some region gets exactly 128 from every replica.
All inputs are finite; a program needn't handle non-finite values.
Results may differ from the reference program's by a relative error of at most 0.011.
Values may be sent and summed in bfloat16 or wider, within the bound.
A program may use at most 128 MiB of HBM per device.

```python
import jax
import jax.numpy as jnp
from jax import lax

D = 8192
BLK = 128
KEEP = 512
HK = 640
TOKENS = 4096
NBLK = 40960
NBS = 10240
REGION_MAX = 1920
N_REP = 8
N_SHARD = 4


def paired(seed_key, center, spread, count, lead_owner):
    key_perm, key_step = jax.random.split(seed_key)
    serial = jax.random.permutation(key_perm, count).astype(jnp.int32)
    first_id = serial[0]
    serial = jnp.where(serial == lead_owner, first_id, serial)
    serial = serial.at[0].set(lead_owner)
    halves = count // 2
    spreads = jax.random.randint(key_step, (halves,), 0, spread + 1).astype(jnp.int32)
    spreads = spreads.at[0].set(spread)
    values = jnp.concatenate([center + spreads, center - spreads]).astype(jnp.int32)
    return jnp.zeros((count,), jnp.int32).at[serial].set(values)


def layout(seed_key):
    base_key = jax.random.fold_in(seed_key, 7301)
    block_count = NBLK // N_SHARD
    mean_len = block_count // N_REP
    shard_keys = jax.random.split(jax.random.fold_in(base_key, 1), N_SHARD)
    lead_len = jax.random.randint(jax.random.fold_in(base_key, 2), (N_SHARD,), 0, N_REP).astype(jnp.int32)

    def one_shard(shard_key, lead_owner):
        return paired(shard_key, mean_len, mean_len // 2, N_REP, lead_owner)
    lengths = jax.vmap(one_shard)(shard_keys, lead_len)
    starts = (jnp.cumsum(lengths, axis=1) - lengths).astype(jnp.int32)
    lead_take = jax.random.randint(jax.random.fold_in(base_key, 3), (N_SHARD,), 0, N_REP).astype(jnp.int32)
    per_owner = KEEP // N_REP
    row_keys = jax.random.split(jax.random.fold_in(base_key, 4), N_REP * N_SHARD)
    shard_of = jnp.arange(N_REP * N_SHARD, dtype=jnp.int32) % N_SHARD

    def pick(row_key, shard):
        key_first, key_second, key_third = jax.random.split(row_key, 3)
        counts = paired(key_first, per_owner, per_owner, N_REP, lead_take[shard])
        start_row = starts[shard]
        blocks = jnp.arange(block_count, dtype=jnp.int32)
        region = (jnp.searchsorted(start_row, blocks, side='right') - 1).astype(jnp.int32)
        noise = jax.random.permutation(key_second, block_count).astype(jnp.int32)
        serial = jnp.argsort(region * block_count + noise, stable=True).astype(jnp.int32)
        region_sorted = region[serial]
        region_rank = jnp.arange(block_count, dtype=jnp.int32) - start_row[region_sorted]
        keep_flags = region_rank < counts[region_sorted]
        picked = jnp.argsort(jnp.where(keep_flags, 0, 1).astype(jnp.int32), stable=True)[:KEEP]
        chosen = serial[picked]
        return chosen[jax.random.permutation(key_third, KEEP)].astype(jnp.int32)
    kept = jax.vmap(pick)(row_keys, shard_of).reshape(N_REP, N_SHARD, KEEP)
    return (lengths, kept)


def draw_region_len(key, part):
    return layout(key)[0]


def draw_kept(key, part):
    return layout(key)[1]


def block_scale(key, dims, cuts, smallest, high):
    gain, own = 1.0, jax.random.fold_in(key, 6)
    for position, parts in cuts:
        heights = jnp.exp(jax.random.uniform(jax.random.fold_in(own, position), (parts,), jnp.float32, smallest / len(cuts), high / len(cuts)))
        gain = gain * jnp.repeat(heights, dims[position] // parts).reshape([-1 if axis == position else 1 for axis in range(len(dims))])
    return gain


def normal_values(stream_key, extent, scale, most, shards=(), kind=jnp.bfloat16):
    drawn = scale * jax.random.normal(stream_key, extent, jnp.float32)
    if shards:
        drawn = drawn * block_scale(stream_key, extent, shards, -0.22, 0.18)
    return jnp.clip(drawn, -most, most).astype(kind)


def setup_inputs(seed: int = 0) -> dict:
    splits = jax.random.split(jax.random.key(seed), 7)
    activ = normal_values(splits[0], (TOKENS, D), 1.0, 6.0, ((0, 32),))
    key_grad = normal_values(splits[1], (TOKENS, HK), 0.2, 1.1953125, ((0, 32),))
    key_weight = normal_values(splits[2], (D, HK), HK ** -0.5, 0.25, ((0, 4),))
    feedback = normal_values(splits[3], (N_REP, NBLK, BLK), 4.0, 24.0, ((0, 8), (1, 4)))
    kept = draw_kept(jax.random.fold_in(splits[6], 71), 0)
    region_len = draw_region_len(jax.random.fold_in(splits[6], 71), 0)
    return {"activ": activ, "key_grad": key_grad, "key_weight": key_weight, "feedback": feedback, "kept": kept, "region_len": region_len}


def reference(activ, key_grad, key_weight, feedback, kept, region_len):
    input_grad = jnp.dot(key_grad, key_weight.T, preferred_element_type=jnp.float32).astype(jnp.bfloat16)
    rep_rows = TOKENS // N_REP
    act_rep = activ.reshape(N_REP, rep_rows, D)
    grad_rep = key_grad.reshape(N_REP, rep_rows, HK)
    shard_base = (jnp.arange(N_SHARD, dtype=jnp.int32) * NBS)[:, None]

    def renew(bundle):
        act_one, grad_one, fed_one, kept_one = bundle
        weight_grad = jnp.dot(act_one.T, grad_one, preferred_element_type=jnp.float32)
        flat_ids = (kept_one + shard_base).reshape(-1).astype(jnp.int32)
        chosen = jnp.zeros((NBLK,), bool).at[flat_ids].set(True)
        cleared = jnp.where(chosen[:, None], jnp.float32(0.0), fed_one.astype(jnp.float32))
        return (cleared + weight_grad.reshape(NBLK, BLK)).astype(jnp.bfloat16)

    next_feedback = lax.map(renew, (act_rep, grad_rep, feedback, kept))

    def fetch(fed_one, kept_one):
        return fed_one[(kept_one + shard_base).reshape(-1).astype(jnp.int32)]

    kept_values = jax.vmap(fetch)(feedback, kept).reshape(N_REP, N_SHARD, KEEP, BLK).astype(jnp.float32)
    starts = (jnp.cumsum(region_len, axis=1) - region_len).astype(jnp.int32)

    def collect(bundle):
        values_one, kept_shard, start_row = bundle
        owner_id = jnp.sum((start_row[None, None, :] <= kept_shard[:, :, None]).astype(jnp.int32), axis=2).astype(jnp.int32) - 1
        place_at = (owner_id * REGION_MAX + kept_shard - start_row[owner_id]).astype(jnp.int32)
        blank = jnp.zeros((N_REP * REGION_MAX, BLK), jnp.float32)
        return blank.at[place_at.reshape(-1)].add(values_one.reshape(-1, BLK))

    owned_sum = lax.map(collect, (jnp.swapaxes(kept_values, 0, 1), jnp.swapaxes(kept, 0, 1), starts))
    return input_grad, next_feedback, owned_sum
```

```python
import functools

import jax
import jax.numpy as jnp
from jax import lax
from jax.experimental import pallas as pl
from jax.experimental.pallas import tpu as pltpu
from jax.sharding import PartitionSpec as P

MESH = pl.DeviceIdType.MESH


def flip(index, bit):
    out = index
    power = 1
    while power <= bit:
        if bit & power:
            out = out + power - 2 * power * ((index // power) % 2)
        power *= 2
    return out


def largest_divisor(total, most, step):
    best = step
    for size in range(step, most + 1, step):
        if total % size == 0:
            best = size
    return best


def kernel(
    n,
    reps,
    activ,
    key_grad,
    key_weight,
    feedback,
    chosen,
    lengths,
    input_grad,
    next_feedback,
    owned,
    grads,
    acts,
    weight,
    table,
    got_rows,
    got_ids,
    cols_out,
    columns_of,
    picked,
    grad_blocks,
    owned_buf,
    local_sem,
    grad_send,
    grad_recv,
    act_send,
    act_recv,
    out_send,
    out_recv,
    row_send,
    row_recv,
    id_send,
    id_recv,
):
    me = lax.axis_index("shard")
    rep = lax.axis_index("rep")
    tokens, feats = key_grad.shape
    width = activ.shape[1] // n
    count, size = table.shape
    keep = chosen.shape[-1]
    masks = list(range(n - 1, 0, -1))

    loads = [
        pltpu.make_async_copy(feedback.at[0], table, local_sem.at[0]),
        pltpu.make_async_copy(key_weight, weight, local_sem.at[1]),
        pltpu.make_async_copy(key_grad, grads.at[me], local_sem.at[2]),
        pltpu.make_async_copy(
            activ.at[:, pl.ds(pl.multiple_of(me * width, width), width)],
            acts.at[me],
            local_sem.at[3],
        ),
    ]
    for load in loads:
        load.start()

    barrier = pltpu.get_barrier_semaphore()
    for mask in masks:
        pl.semaphore_signal(
            barrier, inc=1, device_id={"shard": flip(me, mask)}, device_id_type=MESH
        )
    for d in range(1, reps):
        pl.semaphore_signal(
            barrier, inc=1, device_id={"rep": lax.rem(rep + d, reps)}, device_id_type=MESH
        )
    pl.semaphore_wait(barrier, n - 1 + reps - 1)

    def grad_copy(have, bit):
        block = flip(me, have)
        return pltpu.make_async_remote_copy(
            src_ref=grads.at[block] if have else key_grad,
            dst_ref=grads.at[block],
            send_sem=grad_send.at[have + bit],
            recv_sem=grad_recv.at[have + bit],
            device_id={"shard": flip(me, bit)},
            device_id_type=MESH,
        )

    bits = []
    bit = n // 2
    while bit:
        bits.append(bit)
        bit //= 2
    first = grad_copy(0, bits[0])
    first.start()
    act_copies = []
    for mask in sorted(masks, key=lambda m: m == bits[0] + 1):
        peer = flip(me, mask)
        act_copies.append(
            pltpu.make_async_remote_copy(
                src_ref=activ.at[:, pl.ds(pl.multiple_of(peer * width, width), width)],
                dst_ref=acts.at[me],
                send_sem=act_send.at[mask],
                recv_sem=act_recv.at[mask],
                device_id={"shard": peer},
                device_id_type=MESH,
            )
        )
        act_copies[-1].start()
    id_copies = []
    for d in range(1, reps):
        id_copies.append(
            pltpu.make_async_remote_copy(
                src_ref=chosen.at[0],
                dst_ref=got_ids.at[rep],
                send_sem=id_send.at[d],
                recv_sem=id_recv.at[d],
                device_id={"rep": lax.rem(rep + d, reps)},
                device_id_type=MESH,
            )
        )
        id_copies[-1].start()

    ids_row = chosen[0]
    got_ids[rep] = ids_row
    spread = jnp.broadcast_to(ids_row.astype(jnp.float32), (size, keep))
    columns_of[...] = spread.T.astype(jnp.int32)
    picked[...] = jnp.zeros_like(picked)
    loads[0].wait()
    step = 2 * size

    def pick(i, carry):
        base = pl.multiple_of(i * step, step)
        rows = table[pl.ds(base, step), :]
        lane = lax.broadcasted_iota(jnp.int32, (keep, size), 1) + base
        ids = columns_of[...]
        one_hot = jnp.concatenate(
            [
                jnp.where(ids == lane, 1.0, 0.0).astype(jnp.bfloat16),
                jnp.where(ids == lane + size, 1.0, 0.0).astype(jnp.bfloat16),
            ],
            axis=1,
        )
        picked[...] += jnp.dot(one_hot, rows, preferred_element_type=jnp.float32)
        line = lax.broadcasted_iota(jnp.int32, (step, keep), 0) + base
        taken = jnp.max(
            jnp.where(chosen[0] == line, 1.0, 0.0), axis=1, keepdims=True
        )
        cleared = jnp.where(taken > 0.5, 0.0, rows.astype(jnp.float32))
        table[pl.ds(base, step), :] = cleared.astype(jnp.bfloat16)
        return carry

    lax.fori_loop(0, count // step, pick, 0)
    got_rows[rep] = picked[...].astype(jnp.bfloat16)

    loads[2].wait()
    first.wait_recv()
    have, grad_copies = [0, bits[0]], [first]
    for bit in bits[1:]:
        wave = [grad_copy(h, bit) for h in have]
        for copy in wave:
            copy.start()
        for copy in wave:
            copy.wait_recv()
        grad_copies += wave
        have += [h + bit for h in have]

    loads[1].wait()
    part = largest_divisor(width, 512, 128)

    def columns(block, slot):
        def body(i, carry):
            at = pl.multiple_of(i * part, part)
            cols_out[slot, :, pl.ds(at, part)] = lax.dot_general(
                grads[block],
                weight[pl.ds(at, part), :],
                (((1,), (1,)), ((), ())),
                preferred_element_type=jnp.float32,
            ).astype(jnp.bfloat16)
            return carry

        lax.fori_loop(0, width // part, body, 0)

    mine = input_grad.at[:, pl.ds(pl.multiple_of(me * width, width), width)]
    for mask in masks:
        columns(flip(me, mask), mask)
    row_copies = []
    for d in range(1, reps):
        row_copies.append(
            pltpu.make_async_remote_copy(
                src_ref=got_rows.at[rep],
                dst_ref=got_rows.at[rep],
                send_sem=row_send.at[d],
                recv_sem=row_recv.at[d],
                device_id={"rep": lax.rem(rep + d, reps)},
                device_id_type=MESH,
            )
        )
        row_copies[-1].start()
    columns(me, 0)
    out_copies = []
    for mask in masks:
        out_copies.append(
            pltpu.make_async_remote_copy(
                src_ref=cols_out.at[mask],
                dst_ref=mine,
                send_sem=out_send.at[mask],
                recv_sem=out_recv.at[mask],
                device_id={"shard": flip(me, mask)},
                device_id_type=MESH,
            )
        )
        out_copies[-1].start()
    own_out = pltpu.make_async_copy(cols_out.at[0], mine, local_sem.at[1])
    own_out.start()

    for copy in id_copies:
        copy.wait_recv()
    for copy in row_copies:
        copy.wait_recv()
    lens = lengths[...]
    order = lax.broadcasted_iota(jnp.int32, lens.shape, 1)
    start = jnp.sum(jnp.where(order < rep, lens, 0), axis=1, keepdims=True)
    length = jnp.sum(jnp.where(order == rep, lens, 0), axis=1, keepdims=True)
    region = owned.shape[1]
    tall = largest_divisor(region, 256, 8)

    def gather_region(i, carry):
        base = pl.multiple_of(i * tall, 8)
        line = lax.broadcasted_iota(jnp.int32, (tall, keep), 0) + base

        def add(r, total):
            offset = got_ids[r] - start
            offset = jnp.where((offset >= 0) & (offset < length), offset, -1)
            one_hot = jnp.where(offset == line, 1.0, 0.0).astype(jnp.bfloat16)
            return total + jnp.dot(one_hot, got_rows[r], preferred_element_type=jnp.float32)

        owned_buf[pl.ds(base, tall), :] = lax.fori_loop(
            0, reps, add, jnp.zeros((tall, size), jnp.float32)
        )
        return carry

    lax.fori_loop(0, region // tall, gather_region, 0)
    own_sum = pltpu.make_async_copy(owned_buf, owned.at[0], local_sem.at[0])
    own_sum.start()

    loads[3].wait()
    for copy in act_copies:
        copy.wait_recv()
    chunk = largest_divisor(width, 256, 128)
    per_row = feats // size

    def update(i, carry):
        at = pl.multiple_of(i * chunk, chunk)
        left = acts[:, :, pl.ds(at, chunk)].reshape(n * tokens, chunk)
        right = grads[...].reshape(n * tokens, feats)
        grad = lax.dot_general(
            left, right, (((0,), (0,)), ((), ())), preferred_element_type=jnp.float32
        )
        for j in range(per_row):
            grad_blocks[pl.ds(j, chunk, stride=per_row), :] = grad[:, j * size : (j + 1) * size]
        rows = pl.ds(pl.multiple_of(i * chunk * per_row, chunk * per_row), chunk * per_row)
        table[rows, :] = (table[rows, :].astype(jnp.float32) + grad_blocks[...]).astype(
            jnp.bfloat16
        )
        return carry

    lax.fori_loop(0, width // chunk, update, 0)
    new_table = pltpu.make_async_copy(table, next_feedback.at[0], local_sem.at[2])
    new_table.start()

    own_out.wait()
    own_sum.wait()
    for copy in out_copies:
        copy.wait_recv()
    new_table.wait()
    for copy in grad_copies + act_copies + id_copies + row_copies + out_copies:
        copy.wait_send()


def solution(mesh):
    n, reps = mesh.shape["shard"], mesh.shape["rep"]

    def per_device(activ, key_grad, key_weight, feedback, kept, region_len):
        tokens, feats = key_grad.shape
        width = activ.shape[1] // n
        _, count, size = feedback.shape
        keep = kept.shape[-1]
        mean_len = count // reps
        region = mean_len + mean_len // 2
        dma = pltpu.SemaphoreType.DMA
        any_space = pl.BlockSpec(memory_space=pl.ANY)
        vmem = pl.BlockSpec(memory_space=pltpu.VMEM)
        bf16 = jnp.bfloat16
        return pl.pallas_call(
            functools.partial(kernel, n, reps),
            out_shape=(
                jax.ShapeDtypeStruct(activ.shape, bf16),
                jax.ShapeDtypeStruct(feedback.shape, bf16),
                jax.ShapeDtypeStruct((1, region, size), jnp.float32),
            ),
            in_specs=[any_space] * 4 + [vmem] * 2,
            out_specs=(any_space,) * 3,
            scratch_shapes=[
                pltpu.VMEM((n, tokens, feats), bf16),
                pltpu.VMEM((n, tokens, width), bf16),
                pltpu.VMEM((width, feats), bf16),
                pltpu.VMEM((count, size), bf16),
                pltpu.VMEM((reps, keep, size), bf16),
                pltpu.VMEM((reps, 1, keep), jnp.int32),
                pltpu.VMEM((n, tokens, width), bf16),
                pltpu.VMEM((keep, size), jnp.int32),
                pltpu.VMEM((keep, size), jnp.float32),
                pltpu.VMEM((largest_divisor(width, 256, 128) * (feats // size), size), jnp.float32),
                pltpu.VMEM((region, size), jnp.float32),
                dma((4,)),
                dma((n,)),
                dma((n,)),
                dma((n,)),
                dma((n,)),
                dma((n,)),
                dma((n,)),
                dma((reps,)),
                dma((reps,)),
                dma((reps,)),
                dma((reps,)),
            ],
            compiler_params=pltpu.CompilerParams(
                collective_id=0, has_side_effects=True, vmem_limit_bytes=48 * 1024 * 1024
            ),
        )(activ, key_grad, key_weight, feedback, kept, region_len)

    return jax.shard_map(
        per_device,
        mesh=mesh,
        in_specs=(
            P(("rep", "shard"), None),
            P(("rep", "shard"), None),
            P("shard", None),
            P("rep", "shard", None),
            P("rep", "shard", None),
            P("shard", None),
        ),
        out_specs=(P(("rep", "shard"), None), P("rep", "shard", None), P("shard", "rep", None)),
        check_vma=False,
    )
```

```python
import functools

import jax
import jax.numpy as jnp
from jax import lax
from jax.experimental import pallas as pl
from jax.experimental.pallas import tpu as pltpu
from jax.sharding import PartitionSpec as P

MESH = pl.DeviceIdType.MESH


def flip(index, bit):
    out = index
    power = 1
    while power <= bit:
        if bit & power:
            out = out + power - 2 * power * ((index // power) % 2)
        power *= 2
    return out


def largest_divisor(total, most, step):
    best = step
    for size in range(step, most + 1, step):
        if total % size == 0:
            best = size
    return best


def kernel(
    n,
    reps,
    activ,
    key_grad,
    key_weight,
    feedback,
    kept,
    region_len,
    input_grad,
    next_feedback,
    owned,
    grads,
    acts,
    weight,
    table,
    got_rows,
    got_ids,
    cols_out,
    columns_of,
    picked,
    chosen,
    lengths,
    grad_blocks,
    owned_buf,
    local_sem,
    grad_send,
    grad_recv,
    act_send,
    act_recv,
    out_send,
    out_recv,
    row_send,
    row_recv,
    id_send,
    id_recv,
):
    me = lax.axis_index("shard")
    rep = lax.axis_index("rep")
    tokens, feats = key_grad.shape
    width = activ.shape[1] // n
    count, size = table.shape
    keep = kept.shape[-1]
    masks = list(range(n - 1, 0, -1))

    loads = [
        pltpu.make_async_copy(feedback.at[0], table, local_sem.at[0]),
        pltpu.make_async_copy(key_weight, weight, local_sem.at[1]),
        pltpu.make_async_copy(key_grad, grads.at[me], local_sem.at[2]),
        pltpu.make_async_copy(
            activ.at[:, pl.ds(pl.multiple_of(me * width, width), width)],
            acts.at[me],
            local_sem.at[3],
        ),
        pltpu.make_async_copy(kept.at[0], chosen, local_sem.at[5]),
        pltpu.make_async_copy(region_len, lengths, local_sem.at[6]),
    ]
    for load in loads:
        load.start()

    barrier = pltpu.get_barrier_semaphore()
    for mask in masks:
        pl.semaphore_signal(
            barrier, inc=1, device_id={"shard": flip(me, mask)}, device_id_type=MESH
        )
    for d in range(1, reps):
        pl.semaphore_signal(
            barrier, inc=1, device_id={"rep": lax.rem(rep + d, reps)}, device_id_type=MESH
        )
    pl.semaphore_wait(barrier, n - 1 + reps - 1)

    def grad_copy(have, bit):
        block = flip(me, have)
        return pltpu.make_async_remote_copy(
            src_ref=grads.at[block] if have else key_grad,
            dst_ref=grads.at[block],
            send_sem=grad_send.at[have + bit],
            recv_sem=grad_recv.at[have + bit],
            device_id={"shard": flip(me, bit)},
            device_id_type=MESH,
        )

    bits = []
    bit = n // 2
    while bit:
        bits.append(bit)
        bit //= 2
    first = grad_copy(0, bits[0])
    first.start()
    act_copies = []
    for mask in sorted(masks, key=lambda m: m == bits[0] + 1):
        peer = flip(me, mask)
        act_copies.append(
            pltpu.make_async_remote_copy(
                src_ref=activ.at[:, pl.ds(pl.multiple_of(peer * width, width), width)],
                dst_ref=acts.at[me],
                send_sem=act_send.at[mask],
                recv_sem=act_recv.at[mask],
                device_id={"shard": peer},
                device_id_type=MESH,
            )
        )
        act_copies[-1].start()
    id_copies = []
    for d in range(1, reps):
        id_copies.append(
            pltpu.make_async_remote_copy(
                src_ref=kept.at[0, 0],
                dst_ref=got_ids.at[rep, 0],
                send_sem=id_send.at[d],
                recv_sem=id_recv.at[d],
                device_id={"rep": lax.rem(rep + d, reps)},
                device_id_type=MESH,
            )
        )
        id_copies[-1].start()

    loads[4].wait()
    loads[5].wait()
    ids_row = chosen[...]
    got_ids[rep] = ids_row
    spread = jnp.broadcast_to(ids_row.astype(jnp.float32), (size, keep))
    columns_of[...] = spread.T.astype(jnp.int32)
    picked[...] = jnp.zeros_like(picked)
    loads[0].wait()
    step = 2 * size

    def pick(i, carry):
        base = pl.multiple_of(i * step, step)
        rows = table[pl.ds(base, step), :]
        lane = lax.broadcasted_iota(jnp.int32, (keep, size), 1) + base
        ids = columns_of[...]
        one_hot = jnp.concatenate(
            [
                jnp.where(ids == lane, 1.0, 0.0).astype(jnp.bfloat16),
                jnp.where(ids == lane + size, 1.0, 0.0).astype(jnp.bfloat16),
            ],
            axis=1,
        )
        picked[...] += jnp.dot(one_hot, rows, preferred_element_type=jnp.float32)
        line = lax.broadcasted_iota(jnp.int32, (step, keep), 0) + base
        taken = jnp.max(
            jnp.where(chosen[...] == line, 1.0, 0.0), axis=1, keepdims=True
        )
        cleared = jnp.where(taken > 0.5, 0.0, rows.astype(jnp.float32))
        table[pl.ds(base, step), :] = cleared.astype(jnp.bfloat16)
        return carry

    lax.fori_loop(0, count // step, pick, 0)
    got_rows[rep] = picked[...].astype(jnp.bfloat16)

    loads[2].wait()
    first.wait_recv()
    have, grad_copies = [0, bits[0]], [first]
    for bit in bits[1:]:
        wave = [grad_copy(h, bit) for h in have]
        for copy in wave:
            copy.start()
        for copy in wave:
            copy.wait_recv()
        grad_copies += wave
        have += [h + bit for h in have]

    row_copies = []
    for d in range(1, reps):
        row_copies.append(
            pltpu.make_async_remote_copy(
                src_ref=got_rows.at[rep],
                dst_ref=got_rows.at[rep],
                send_sem=row_send.at[d],
                recv_sem=row_recv.at[d],
                device_id={"rep": lax.rem(rep + d, reps)},
                device_id_type=MESH,
            )
        )
        row_copies[-1].start()

    loads[1].wait()
    part = largest_divisor(width, 512, 128)

    def columns(block, slot):
        def body(i, carry):
            at = pl.multiple_of(i * part, part)
            cols_out[slot, :, pl.ds(at, part)] = lax.dot_general(
                grads[block],
                weight[pl.ds(at, part), :],
                (((1,), (1,)), ((), ())),
                preferred_element_type=jnp.float32,
            ).astype(jnp.bfloat16)
            return carry

        lax.fori_loop(0, width // part, body, 0)

    mine = input_grad.at[:, pl.ds(pl.multiple_of(me * width, width), width)]
    for mask in masks:
        columns(flip(me, mask), mask)
    columns(me, 0)
    out_copies = []
    for mask in masks:
        out_copies.append(
            pltpu.make_async_remote_copy(
                src_ref=cols_out.at[mask],
                dst_ref=mine,
                send_sem=out_send.at[mask],
                recv_sem=out_recv.at[mask],
                device_id={"shard": flip(me, mask)},
                device_id_type=MESH,
            )
        )
        out_copies[-1].start()
    own_out = pltpu.make_async_copy(cols_out.at[0], mine, local_sem.at[1])
    own_out.start()

    loads[3].wait()
    for copy in act_copies:
        copy.wait_recv()
    chunk = largest_divisor(width, 256, 128)
    per_row = feats // size

    def update(i, carry):
        at = pl.multiple_of(i * chunk, chunk)
        left = acts[:, :, pl.ds(at, chunk)].reshape(n * tokens, chunk)
        right = grads[...].reshape(n * tokens, feats)
        grad = lax.dot_general(
            left, right, (((0,), (0,)), ((), ())), preferred_element_type=jnp.float32
        )
        for j in range(per_row):
            grad_blocks[pl.ds(j, chunk, stride=per_row), :] = grad[:, j * size : (j + 1) * size]
        rows = pl.ds(pl.multiple_of(i * chunk * per_row, chunk * per_row), chunk * per_row)
        table[rows, :] = (table[rows, :].astype(jnp.float32) + grad_blocks[...]).astype(
            jnp.bfloat16
        )
        return carry

    lax.fori_loop(0, width // chunk, update, 0)
    new_table = pltpu.make_async_copy(table, next_feedback.at[0], local_sem.at[2])
    new_table.start()

    for copy in id_copies:
        copy.wait_recv()
    for copy in row_copies:
        copy.wait_recv()
    lens = lengths[...]
    order = lax.broadcasted_iota(jnp.int32, lens.shape, 1)
    start = jnp.sum(jnp.where(order < rep, lens, 0), axis=1, keepdims=True)
    length = jnp.sum(jnp.where(order == rep, lens, 0), axis=1, keepdims=True)
    region = owned.shape[1]
    tall = largest_divisor(region, 256, 8)

    def gather_region(i, carry):
        base = pl.multiple_of(i * tall, 8)
        line = lax.broadcasted_iota(jnp.int32, (tall, keep), 0) + base

        def add(r, total):
            offset = got_ids[r] - start
            offset = jnp.where((offset >= 0) & (offset < length), offset, -1)
            one_hot = jnp.where(offset == line, 1.0, 0.0).astype(jnp.bfloat16)
            return total + jnp.dot(one_hot, got_rows[r], preferred_element_type=jnp.float32)

        owned_buf[pl.ds(base, tall), :] = lax.fori_loop(
            0, reps, add, jnp.zeros((tall, size), jnp.float32)
        )
        return carry

    lax.fori_loop(0, region // tall, gather_region, 0)
    own_sum = pltpu.make_async_copy(owned_buf, owned.at[0], local_sem.at[0])
    own_sum.start()

    own_out.wait()
    own_sum.wait()
    for copy in out_copies:
        copy.wait_recv()
    new_table.wait()
    for copy in grad_copies + act_copies + id_copies + row_copies + out_copies:
        copy.wait_send()


def solution(mesh):
    n, reps = mesh.shape["shard"], mesh.shape["rep"]

    def per_device(activ, key_grad, key_weight, feedback, kept, region_len):
        tokens, feats = key_grad.shape
        width = activ.shape[1] // n
        _, count, size = feedback.shape
        keep = kept.shape[-1]
        mean_len = count // reps
        region = mean_len + mean_len // 2
        dma = pltpu.SemaphoreType.DMA
        any_space = pl.BlockSpec(memory_space=pl.ANY)
        bf16 = jnp.bfloat16
        return pl.pallas_call(
            functools.partial(kernel, n, reps),
            out_shape=(
                jax.ShapeDtypeStruct(activ.shape, bf16),
                jax.ShapeDtypeStruct(feedback.shape, bf16),
                jax.ShapeDtypeStruct((1, region, size), jnp.float32),
            ),
            in_specs=[any_space] * 6,
            out_specs=(any_space,) * 3,
            scratch_shapes=[
                pltpu.VMEM((n, tokens, feats), bf16),
                pltpu.VMEM((n, tokens, width), bf16),
                pltpu.VMEM((width, feats), bf16),
                pltpu.VMEM((count, size), bf16),
                pltpu.VMEM((reps, keep, size), bf16),
                pltpu.VMEM((reps, 1, keep), jnp.int32),
                pltpu.VMEM((n, tokens, width), bf16),
                pltpu.VMEM((keep, size), jnp.int32),
                pltpu.VMEM((keep, size), jnp.float32),
                pltpu.VMEM((1, keep), jnp.int32),
                pltpu.VMEM((1, reps), jnp.int32),
                pltpu.VMEM((largest_divisor(width, 256, 128) * (feats // size), size), jnp.float32),
                pltpu.VMEM((region, size), jnp.float32),
                dma((7,)),
                dma((n,)),
                dma((n,)),
                dma((n,)),
                dma((n,)),
                dma((n,)),
                dma((n,)),
                dma((reps,)),
                dma((reps,)),
                dma((reps,)),
                dma((reps,)),
            ],
            compiler_params=pltpu.CompilerParams(
                collective_id=0, has_side_effects=True, vmem_limit_bytes=67043328
            ),
        )(activ, key_grad, key_weight, feedback, kept, region_len)

    return jax.shard_map(
        per_device,
        mesh=mesh,
        in_specs=(
            P(("rep", "shard"), None),
            P(("rep", "shard"), None),
            P("shard", None),
            P("rep", "shard", None),
            P("rep", "shard", None),
            P("shard", None),
        ),
        out_specs=(P(("rep", "shard"), None), P("rep", "shard", None), P("shard", "rep", None)),
        check_vma=False,
    )
```
